32 devices in a mesh: band: 8 (over y, x, core), grid: 4 (over z).
Axes of the slice: x: 2, y: 2, z: 4, core: 2. Of those that a mesh axis runs over, the one named last changes fastest.
Arguments:
- orbitals: bfloat16 [64, 128, 128, 128], P('band', None, 'grid'), may hold values from -0.75 to 0.75
- occupations: float32 [64], P('band'), may hold values from 0 to 2
- rho_in: float32 [128, 128, 128], P('band', 'grid'), may hold values from 0.5 to 1.5
- hist_in: float32 [7, 128, 128, 128], P(None, 'band', 'grid'), may hold values from 0.5 to 1.5
- hist_res: float32 [7, 128, 128, 128], P(None, 'band', 'grid'), may hold values from -10 to 10
Outputs:
- rho_next: float32 [128, 128, 128], P('band', 'grid')
- v_hartree: float32 [128, 128, 128], P('band', 'grid')
The draws below stay inside these ranges and needn't reach their ends.
All inputs are finite; a program needn't handle non-finite values.
Results may differ from the reference program's by a relative error of at most 0.0003.
Values sent between devices are 32-bit elements; how exact they have to be, the bound alone decides.
A program may use at most 64 MiB of HBM per device.

```python
import jax
import jax.numpy as jnp
from jax import lax

N = 128
HIST = 7
BANDS = 64


def draw_hist_res(key, part):
    base_key = jax.random.fold_in(key, 17)
    key_common, key_own, key_scale = jax.random.split(base_key, 3)
    common = jnp.clip(jax.random.normal(key_common, (N, N, N), jnp.float32), -5.0, 5.0)
    shared = 0.5
    own_part = jnp.clip(jax.random.normal(key_own, (HIST, N, N, N), jnp.float32), -5.0, 5.0)
    scales = jnp.exp(jax.random.uniform(key_scale, (HIST,), jnp.float32, -2.302585, 0.0))
    return scales[:, None, None, None] * (shared * common[None] + own_part)


def level_of(own_key, extent, cuts, least, high):
    def one(axis_at, blocks):
        steps = jax.random.uniform(jax.random.fold_in(jax.random.fold_in(own_key, 6), axis_at), (blocks,), jnp.float32, least / len(cuts), high / len(cuts))
        return jnp.repeat(jnp.exp(steps), extent[axis_at] // blocks).reshape((-1,) + (1,) * (len(extent) - axis_at - 1))

    factor_of = one(*cuts[0])
    for cut in cuts[1:]:
        factor_of = factor_of * one(*cut)
    return factor_of


def bell_draw(key, extent, deviation, limit, pieces=(), kind=jnp.bfloat16):
    drawn = deviation * jax.random.normal(key, extent, jnp.float32)
    if pieces:
        drawn = drawn * level_of(key, extent, pieces, -0.22, 0.18)
    return jnp.clip(drawn, -limit, limit).astype(kind)


def setup_inputs(seed: int = 0) -> dict:
    seeds = jax.random.split(jax.random.key(seed), 6)
    orbitals = bell_draw(seeds[0], (BANDS, N, N, N), BANDS ** -0.5, 0.75, ((0, 8), (2, 4)))
    occupations = jnp.clip(2.0 * jax.random.uniform(seeds[1], (BANDS,), jnp.float32) ** level_of(seeds[1], (BANDS,), ((0, 8),), -0.2, 0.2), 0.0, 2.0)
    rho_in = jnp.clip(0.5 + 1.0 * jax.random.uniform(seeds[2], (N, N, N), jnp.float32) ** level_of(seeds[2], (N, N, N), ((0, 8), (1, 4)), -0.2, 0.2), 0.5, 1.5)
    hist_in = jnp.clip(0.5 + 1.0 * jax.random.uniform(seeds[3], (HIST, N, N, N), jnp.float32) ** level_of(seeds[3], (HIST, N, N, N), ((1, 8), (2, 4)), -0.2, 0.2), 0.5, 1.5)
    hist_res = draw_hist_res(jax.random.fold_in(seeds[5], 71), 0)
    return dict(orbitals=orbitals, occupations=occupations, rho_in=rho_in, hist_in=hist_in, hist_res=hist_res)


beta_mix = 0.5
spacing = 0.2

def coulomb_kernel(length):
    positions = jnp.arange(length, dtype=jnp.int32)
    freq_all = jnp.where(positions < length // 2, positions, positions - length)
    square_all = freq_all * freq_all
    squared_sum = square_all[:, None, None] + square_all[None, :, None] + square_all[None, None, :]
    cell_len = length * spacing
    floored = jnp.maximum(squared_sum, 1).astype(jnp.float32)
    values_all = cell_len * cell_len / jnp.pi / floored
    return jnp.where(squared_sum > 0, values_all, jnp.zeros_like(values_all)).astype(jnp.float32)

def reference(orbitals, occupations, rho_in, hist_in, hist_res):

    def add_band(summed, band_pair):
        orbital, weight = band_pair
        amplitude = orbital.astype(jnp.float32)
        return (summed + weight * amplitude * amplitude, None)
    rho_out, _ = lax.scan(add_band, jnp.zeros((N, N, N), jnp.float32), (orbitals, occupations))
    res_new = rho_out - rho_in
    residuals = jnp.concatenate([hist_res, res_new[None]], axis=0)
    inputs = jnp.concatenate([hist_in, rho_in[None]], axis=0)
    flat_res = residuals.reshape(HIST + 1, N * N * N)
    gram_matrix = jnp.dot(flat_res.astype(jnp.float32), flat_res.T.astype(jnp.float32), precision=lax.Precision.HIGHEST, preferred_element_type=jnp.float32) / (N * N * N)
    factor = jnp.linalg.cholesky(gram_matrix)
    solved = jax.scipy.linalg.cho_solve((factor, True), jnp.ones((HIST + 1,), jnp.float32))
    weights = solved / jnp.sum(solved)
    trials = inputs + beta_mix * residuals
    rho_next = jnp.tensordot(weights, trials, axes=1, precision=lax.Precision.HIGHEST)
    spectrum = jnp.fft.fftn(rho_next)
    v_hartree = jnp.real(jnp.fft.ifftn(spectrum * coulomb_kernel(N))).astype(jnp.float32)
    return (rho_next, v_hartree)
```

```python
import functools

import jax
import jax.numpy as jnp
import numpy as np
from jax import lax
from jax.experimental import pallas as pl
from jax.experimental.pallas import tpu as pltpu
from jax.sharding import PartitionSpec as P

beta_mix = 0.5
spacing = 0.2
MESH = pl.DeviceIdType.MESH
HIGH = lax.Precision.HIGHEST
F32 = jnp.float32


def cas_table(length):
    phases = np.outer(np.arange(length), np.arange(length)) % length
    angles = phases.astype(np.float64) * (2.0 * np.pi / length)
    return (np.cos(angles) + np.sin(angles)).astype(np.float32)


def dot(left, right):
    return jnp.dot(left, right, precision=HIGH, preferred_element_type=F32)


def swap_lane_groups(parts, width):
    count = len(parts)
    total = count * width
    group = lax.broadcasted_iota(jnp.int32, parts[0].shape, 1) // width
    results = []
    for j in range(count):
        result = parts[j]
        for i in range(count):
            if i != j:
                moved = pltpu.roll(parts[i], ((i - j) * width) % total, 1)
                result = jnp.where(group == i, moved, result)
        results.append(result)
    return results


def body(
    nb, ng,
    occ, orb_hbm, rho_hbm, hin_hbm, hres_hbm, cas_ref,
    rho_ref, pot_ref,
    orb, rin, hin, hres, other, own, pair_in, far_in, resn,
    gram_me, gram_b, gram_me2, gram_g, kern,
    zsend, zrecv, vsend, wrecv, wsend, vrecv, z2send, y2recv,
    load_sem, orb_sem,
    pair_s, pair_r, far_s, far_r, gb_s, gb_r, gg_s, gg_r,
    f1_s, f1_r, f2_s, f2_r, b2_s, b2_r, b1_s, b1_r,
):
    me = lax.axis_index("band")
    mg = lax.axis_index("grid")
    bands, rows, cols, n = orb.shape[1], orb.shape[2], orb.shape[3], orb.shape[4]
    hist = hin.shape[0]
    vecs = hist + 1
    chips = nb // 2
    chip, core = me // 2, me % 2
    partner = chip * 2 + (1 - core)
    quad = rows // ng
    width = n // ng
    qper = width // nb
    order = [d for d in range(chips // 2, 0, -1)] + [d for d in range(chips // 2 + 1, chips)] + [0]

    barrier = pltpu.get_barrier_semaphore()
    for k in range(1, nb):
        pl.semaphore_signal(barrier, inc=1, device_id=((me + k) % nb, mg), device_id_type=MESH)
    for k in range(1, ng):
        pl.semaphore_signal(barrier, inc=1, device_id=(me, (mg + k) % ng), device_id_type=MESH)

    def slab_of(t, mine):
        target = (chip + order[t]) % chips
        return target * 2 + (core if mine else 1 - core)

    orb_loads = []
    for t in range(chips):
        for mine in (False, True):
            s = slab_of(t, mine)
            c = pltpu.make_async_copy(
                orb_hbm.at[:, pl.ds(s * rows, rows)], orb.at[2 * t + mine], orb_sem.at[2 * t + mine]
            )
            c.start()
            orb_loads.append(c)
    loads = [
        pltpu.make_async_copy(hres_hbm, hres, load_sem.at[0]),
        pltpu.make_async_copy(hin_hbm, hin, load_sem.at[1]),
        pltpu.make_async_copy(rho_hbm, rin, load_sem.at[2]),
    ]
    for c in loads:
        c.start()

    def density(index, out):
        def row(a, carry):
            total = None
            for k in range(bands):
                o = orb[index, k, a].astype(F32)
                term = occ[k] * (o * o)
                total = term if total is None else total + term
            out[a] = total
            return carry

        lax.fori_loop(0, rows, row, 0)

    pair_copies, far_copies = [], []

    def finish(t):
        pair_copies[t].wait_recv()

        def row(a, carry):
            own[t, a] = own[t, a] + pair_in[t, a]
            return carry

        lax.fori_loop(0, rows, row, 0)
        if order[t]:
            target = (chip + order[t]) % chips
            c = pltpu.make_async_remote_copy(
                src_ref=own.at[t], dst_ref=far_in.at[t], send_sem=far_s.at[t], recv_sem=far_r.at[t],
                device_id=(target * 2 + core, mg), device_id_type=MESH,
            )
            c.start()
            far_copies.append(c)

    for t in range(chips):
        orb_loads[2 * t].wait()
        density(2 * t, other.at[t])
        if t == 0:
            pl.semaphore_wait(barrier, nb - 1 + ng - 1)
        c = pltpu.make_async_remote_copy(
            src_ref=other.at[t], dst_ref=pair_in.at[t], send_sem=pair_s.at[t], recv_sem=pair_r.at[t],
            device_id=(partner, mg), device_id_type=MESH,
        )
        c.start()
        pair_copies.append(c)
        orb_loads[2 * t + 1].wait()
        density(2 * t + 1, own.at[t])
        if t:
            finish(t - 1)
    finish(chips - 1)

    for c in loads:
        c.wait()
    tiles = cols // 8
    pairs = [(i, j) for i in range(hist) for j in range(i, hist)]

    def gram_row(a, accs):
        accs = list(accs)
        for s in range(tiles):
            vals = [hres[i, a, 8 * s:8 * s + 8, :] for i in range(hist)]
            for x, (i, j) in enumerate(pairs):
                accs[x] = accs[x] + vals[i] * vals[j]
        return tuple(accs)

    zero = jnp.zeros((8, n), F32)
    accs = lax.fori_loop(0, rows, gram_row, tuple(zero for _ in pairs))
    line = {p: jnp.sum(accs[x], axis=0, keepdims=True) for x, p in enumerate(pairs)}
    row_id = lax.broadcasted_iota(jnp.int32, (vecs, n), 0)
    col_id = lax.broadcasted_iota(jnp.int32, (vecs, n), 1)

    def stack(lines):
        result = jnp.zeros((vecs, n), F32)
        for i, l in enumerate(lines):
            result = jnp.where(row_id == i, l, result)
        return jnp.sum(result, axis=1, keepdims=True)

    gram = jnp.zeros((vecs, n), F32)
    for j in range(hist):
        column = stack([line[(min(i, j), max(i, j))] for i in range(hist)])
        gram = jnp.where(col_id == j, column, gram)

    def trial_row(a, carry):
        for m in range(hist):
            hin[m, a] = hin[m, a] + beta_mix * hres[m, a]
        return carry

    lax.fori_loop(0, rows, trial_row, 0)

    def freq2(positions):
        f = jnp.where(positions < n // 2, positions, positions - n)
        return f * f

    first = freq2(lax.broadcasted_iota(jnp.int32, (n, n), 0))
    lane = lax.broadcasted_iota(jnp.int32, (n, n), 1)
    last = freq2(mg * width + lane % width)
    cell = n * spacing
    for q in range(qper):
        middle = freq2((lane // width) * width + me * qper + q)
        squared = first + middle + last
        value = (cell * cell / np.pi) / jnp.maximum(squared, 1).astype(F32)
        kern[:, q * n:(q + 1) * n] = jnp.where(squared > 0, value, 0.0) * (1.0 / (n * n * n))

    for c in far_copies:
        c.wait_recv()

    def late_row(a, accs):
        accs = list(accs)
        total = own[chips - 1, a]
        for t in range(chips - 1):
            total = total + far_in[t, a]
        inp = rin[a]
        res = total - inp
        resn[a] = inp + beta_mix * res
        for s in range(tiles):
            r = res[8 * s:8 * s + 8, :]
            for i in range(hist):
                accs[i] = accs[i] + hres[i, a, 8 * s:8 * s + 8, :] * r
            accs[hist] = accs[hist] + r * r
        return tuple(accs)

    accs = lax.fori_loop(0, rows, late_row, tuple(zero for _ in range(vecs)))
    column = stack([jnp.sum(x, axis=0, keepdims=True) for x in accs])
    as_row = jnp.sum(jnp.where(row_id == col_id, column, 0.0), axis=0, keepdims=True)
    gram = jnp.where(col_id == hist, column, gram)
    gram = jnp.where(row_id == hist, as_row, gram)

    def sum_over(value, source, landing, send, recv, count, index, device_of):
        source[...] = value
        copies = []
        for k in range(1, count):
            c = pltpu.make_async_remote_copy(
                src_ref=source, dst_ref=landing.at[k], send_sem=send.at[k], recv_sem=recv.at[k],
                device_id=device_of((index + k) % count), device_id_type=MESH,
            )
            c.start()
            copies.append(c)
        for c in copies:
            c.wait_recv()
        landing[0] = value
        total = jnp.zeros_like(value)
        for k in range(count):
            total = total + landing[(index - k + count) % count]
        return total, copies

    sent = []
    gram, copies = sum_over(gram, gram_me, gram_b, gb_s, gb_r, nb, me, lambda x: (x, mg))
    sent += copies
    gram, copies = sum_over(gram, gram_me2, gram_g, gg_s, gg_r, ng, mg, lambda x: (me, x))
    sent += copies
    gram = gram * (1.0 / (n * n * n))

    system = jnp.where(col_id == vecs, 1.0, gram)
    for k in range(vecs):
        pivot_row = system[k:k + 1, :] / system[k:k + 1, k:k + 1]
        factor = jnp.where(row_id == k, 0.0, jnp.broadcast_to(system[:, k:k + 1], (vecs, n)))
        system = jnp.where(row_id == k, pivot_row, system - factor * pivot_row)
    solved = system[:, vecs:vecs + 1]
    weights = solved / jnp.sum(solved, axis=0, keepdims=True)
    wide = [jnp.broadcast_to(weights[m:m + 1, :], (cols, n)) for m in range(vecs)]

    def mix_row(a, carry):
        total = wide[hist] * resn[a]
        for m in range(hist):
            total = total + wide[m] * hin[m, a]
        rho_ref[a] = total
        return carry

    lax.fori_loop(0, rows, mix_row, 0)

    cas = cas_ref[...]

    def exchange(source, landing, send, recv, count, index, device_of):
        copies = []
        for k in range(1, count):
            to = (index + k) % count
            c = pltpu.make_async_remote_copy(
                src_ref=source.at[to], dst_ref=landing.at[index], send_sem=send.at[k],
                recv_sem=recv.at[k], device_id=device_of(to), device_id_type=MESH,
            )
            c.start()
            copies.append(c)
        landing[index] = source[index]
        for c in copies:
            c.wait_recv()
        return copies

    on_band = lambda x: (x, mg)
    on_grid = lambda x: (me, x)

    spec = dot(rho_ref[...].reshape(rows * cols, n), cas)
    chunk = quad * cols
    parts = swap_lane_groups([spec[i * chunk:(i + 1) * chunk] for i in range(ng)], width)
    for j in range(ng):
        zsend[j] = parts[j]
    sent += exchange(zsend, zrecv, f1_s, f1_r, ng, mg, on_grid)

    for u in range(quad):
        block = jnp.concatenate([zrecv[x, u * cols:(u + 1) * cols, :] for x in range(ng)], axis=0)
        spec = dot(cas, block)
        parts = swap_lane_groups([spec[j * width:(j + 1) * width] for j in range(ng)], width)
        for i in range(ng):
            vsend[:, :, i * quad + u, :] = parts[i].reshape(nb, qper, n)
    sent += exchange(vsend, wrecv, f2_s, f2_r, nb, me, on_band)

    for q in range(qper):
        block = wrecv[:, q].reshape(n, n)
        spec = dot(cas, block) * kern[:, q * n:(q + 1) * n]
        wsend[:, q] = dot(cas, spec).reshape(nb, rows, n)
    sent += exchange(wsend, vrecv, b2_s, b2_r, nb, me, on_band)

    for u in range(quad):
        parts = swap_lane_groups(
            [vrecv[:, :, i * quad + u, :].reshape(width, n) for i in range(ng)], width
        )
        back = dot(cas, jnp.concatenate(parts, axis=0))
        for x in range(ng):
            z2send[x, u * cols:(u + 1) * cols, :] = back[x * cols:(x + 1) * cols]
    sent += exchange(z2send, y2recv, b1_s, b1_r, ng, mg, on_grid)

    parts = swap_lane_groups([y2recv[j] for j in range(ng)], width)
    for i in range(ng):
        pot_ref[i * quad:(i + 1) * quad] = dot(parts[i], cas).reshape(quad, cols, n)

    for c in pair_copies + far_copies + sent:
        c.wait_send()


def local(nb, ng, orbitals, occupations, rho_in, hist_in, hist_res):
    bands = orbitals.shape[0]
    rows, cols, n = rho_in.shape
    hist = hist_in.shape[0]
    vecs = hist + 1
    chips = nb // 2
    width = n // ng
    qper = width // nb
    quad = rows // ng
    dma = pltpu.SemaphoreType.DMA
    vmem = lambda *shape: pltpu.VMEM(shape, F32)
    anywhere = pl.BlockSpec(memory_space=pl.ANY)
    block = jax.ShapeDtypeStruct((rows, cols, n), F32)
    return pl.pallas_call(
        functools.partial(body, nb, ng),
        out_shape=(block, block),
        in_specs=[pl.BlockSpec(memory_space=pltpu.SMEM)] + [anywhere] * 4 + [pl.BlockSpec(memory_space=pltpu.VMEM)],
        out_specs=(pl.BlockSpec(memory_space=pltpu.VMEM),) * 2,
        scratch_shapes=[
            pltpu.VMEM((nb, bands, rows, cols, n), orbitals.dtype),
            vmem(rows, cols, n),
            vmem(hist, rows, cols, n),
            vmem(hist, rows, cols, n),
            vmem(chips, rows, cols, n),
            vmem(chips, rows, cols, n),
            vmem(chips, rows, cols, n),
            vmem(chips, rows, cols, n),
            vmem(rows, cols, n),
            vmem(vecs, n),
            vmem(nb, vecs, n),
            vmem(vecs, n),
            vmem(ng, vecs, n),
            vmem(n, qper * n),
            vmem(ng, quad * cols, n),
            vmem(ng, quad * cols, n),
            vmem(nb, qper, rows, n),
            vmem(nb, qper, rows, n),
            vmem(nb, qper, rows, n),
            vmem(nb, qper, rows, n),
            vmem(ng, quad * cols, n),
            vmem(ng, quad * cols, n),
            dma((3,)), dma((nb,)),
            dma((chips,)), dma((chips,)), dma((chips,)), dma((chips,)),
            dma((nb,)), dma((nb,)), dma((ng,)), dma((ng,)),
            dma((ng,)), dma((ng,)), dma((nb,)), dma((nb,)),
            dma((nb,)), dma((nb,)), dma((ng,)), dma((ng,)),
        ],
        compiler_params=pltpu.CompilerParams(collective_id=0, has_side_effects=True, vmem_limit_bytes=48 * 1024 * 1024),
        name="density_mix_hartree",
    )(occupations, orbitals, rho_in, hist_in, hist_res, jnp.asarray(cas_table(n)))


def solution(mesh):
    return jax.shard_map(
        functools.partial(local, mesh.shape["band"], mesh.shape["grid"]),
        mesh=mesh,
        in_specs=(
            P("band", None, "grid", None),
            P("band"),
            P("band", "grid", None),
            P(None, "band", "grid", None),
            P(None, "band", "grid", None),
        ),
        out_specs=(P("band", "grid", None), P("band", "grid", None)),
        check_vma=False,
    )
```

```python
import functools

import jax
import jax.numpy as jnp
import numpy as np
from jax import lax
from jax.experimental import pallas as pl
from jax.experimental.pallas import tpu as pltpu
from jax.sharding import PartitionSpec as P

beta_mix = 0.5
spacing = 0.2
MESH = pl.DeviceIdType.MESH
HIGH = lax.Precision.HIGHEST
F32 = jnp.float32


def cas_table(length):
    phases = np.outer(np.arange(length), np.arange(length)) % length
    angles = phases.astype(np.float64) * (2.0 * np.pi / length)
    return (np.cos(angles) + np.sin(angles)).astype(np.float32)


def dot(left, right):
    return jnp.dot(left, right, precision=HIGH, preferred_element_type=F32)


def swap_lane_groups(parts, width):
    count = len(parts)
    total = count * width
    group = lax.broadcasted_iota(jnp.int32, parts[0].shape, 1) // width
    step = 1
    while step < count:
        odd = (group // step) % 2 == 1
        mixed = []
        for i in range(count):
            if (i // step) % 2 == 0:
                mixed.append(jnp.where(odd, pltpu.roll(parts[i + step], step * width, 1), parts[i]))
            else:
                mixed.append(jnp.where(odd, parts[i], pltpu.roll(parts[i - step], total - step * width, 1)))
        parts = mixed
        step *= 2
    return parts


def body(
    nb, ng,
    occ, orb_hbm, rho_hbm, hin_hbm, hres_hbm, cas_hbm,
    rho_ref, pot_ref,
    orb, rin, cas_ref, hin, hres, other, own, pair_in, far_in, relay_in, resn,
    gram_me, gram_b, gram_me2, gram_g, kern,
    zsend, zrecv, vsend, wrecv, wsend, vrecv, z2send, y2recv,
    load_sem, orb_sem,
    pair_s, pair_r, far_s, far_r, gb_s, gb_r, gg_s, gg_r,
    f1_s, f1_r, f2_s, f2_r, b2_s, b2_r, b1_s, b1_r,
):
    me = lax.axis_index("band")
    mg = lax.axis_index("grid")
    bands, rows, cols, n = orb.shape[1], orb.shape[2], orb.shape[3], orb.shape[4]
    hist = hin.shape[0]
    vecs = hist + 1
    chips = nb // 2
    chip, core = me // 2, me % 2
    partner = chip * 2 + (1 - core)
    chunks, width = cuts(nb, ng, rows, n)
    groups = ng * chunks
    quad = rows // groups
    qper = width // nb
    square = chips == 4
    order = [d for d in range(chips // 2, 0, -1)] + [d for d in range(chips // 2 + 1, chips)] + [0]

    barrier = pltpu.get_barrier_semaphore()
    for k in range(1, nb):
        pl.semaphore_signal(barrier, inc=1, device_id=((me + k) % nb, mg), device_id_type=MESH)
    for k in range(1, ng):
        pl.semaphore_signal(barrier, inc=1, device_id=(me, (mg + k) % ng), device_id_type=MESH)

    chip_y, chip_x = chip // 2, chip % 2
    x_chip, y_chip = chip_y * 2 + 1 - chip_x, (1 - chip_y) * 2 + chip_x
    opposite = (1 - chip_y) * 2 + 1 - chip_x

    def target_of(t):
        return (opposite, x_chip, y_chip, chip)[t] if square else (chip + order[t]) % chips

    def slab_of(t, mine):
        target = target_of(t)
        return target * 2 + (core if mine else 1 - core)

    orb_loads = []
    for t in range(chips):
        for mine in (False, True):
            s = slab_of(t, mine)
            c = pltpu.make_async_copy(
                orb_hbm.at[:, pl.ds(s * rows, rows)], orb.at[2 * t + mine], orb_sem.at[2 * t + mine]
            )
            c.start()
            orb_loads.append(c)
    loads = [
        pltpu.make_async_copy(hres_hbm, hres, load_sem.at[0]),
        pltpu.make_async_copy(hin_hbm, hin, load_sem.at[1]),
        pltpu.make_async_copy(rho_hbm, rin, load_sem.at[2]),
        pltpu.make_async_copy(cas_hbm, cas_ref, load_sem.at[3]),
    ]
    for c in loads:
        c.start()

    def density(index, out):
        def row(a, carry):
            total = None
            for k in range(bands):
                o = orb[index, k, a].astype(F32)
                term = occ[k] * (o * o)
                total = term if total is None else total + term
            out[a] = total
            return carry

        lax.fori_loop(0, rows, row, 0)

    pair_copies, far_copies = [], []

    def finish(t):
        pair_copies[t].wait_recv()

        def row(a, carry):
            own[t, a] = own[t, a] + pair_in[t, a]
            return carry

        lax.fori_loop(0, rows, row, 0)
        if square:
            if t == 0:
                far(own.at[0, :half], relay_in.at[0], 0, x_chip)
                far(own.at[0, half:], relay_in.at[1], 1, y_chip)
            if t == 1:
                far(own.at[1, :half], far_in.at[0, :half], 2, x_chip)
            if t == 2:
                far(own.at[2, half:], far_in.at[1, half:], 3, y_chip)
        elif order[t]:
            far(own.at[t], far_in.at[t], t, target_of(t))

    half = rows // 2

    def far(source, landing, slot, target):
        c = pltpu.make_async_remote_copy(
            src_ref=source, dst_ref=landing, send_sem=far_s.at[slot], recv_sem=far_r.at[slot],
            device_id=(target * 2 + core, mg), device_id_type=MESH,
        )
        c.start()
        far_copies.append(c)

    def relay():
        def add(side, slab, base):
            def row(a, carry):
                own[slab, base + a] = own[slab, base + a] + relay_in[side, a]
                return carry

            lax.fori_loop(0, half, row, 0)

        far_copies[1].wait_recv()
        add(1, 1, half)
        far(own.at[1, half:], far_in.at[0, half:], 4, x_chip)
        far_copies[0].wait_recv()
        add(0, 2, 0)
        far(own.at[2, :half], far_in.at[1, :half], 5, y_chip)

    for t in range(chips):
        orb_loads[2 * t].wait()
        density(2 * t, other.at[t])
        if t == 0:
            pl.semaphore_wait(barrier, nb - 1 + ng - 1)
        c = pltpu.make_async_remote_copy(
            src_ref=other.at[t], dst_ref=pair_in.at[t], send_sem=pair_s.at[t], recv_sem=pair_r.at[t],
            device_id=(partner, mg), device_id_type=MESH,
        )
        c.start()
        pair_copies.append(c)
        orb_loads[2 * t + 1].wait()
        density(2 * t + 1, own.at[t])
        if t:
            finish(t - 1)
    finish(chips - 1)
    if square:
        relay()

    for c in loads:
        c.wait()
    tiles = cols // 8
    pairs = [(i, j) for i in range(hist) for j in range(i, hist)]

    def gram_row(a, accs):
        accs = list(accs)
        for s in range(tiles):
            vals = [hres[i, a, 8 * s:8 * s + 8, :] for i in range(hist)]
            for x, (i, j) in enumerate(pairs):
                accs[x] = accs[x] + vals[i] * vals[j]
        return tuple(accs)

    zero = jnp.zeros((8, n), F32)
    accs = lax.fori_loop(0, rows, gram_row, tuple(zero for _ in pairs))
    line = {p: jnp.sum(accs[x], axis=0, keepdims=True) for x, p in enumerate(pairs)}
    row_id = lax.broadcasted_iota(jnp.int32, (vecs, n), 0)
    col_id = lax.broadcasted_iota(jnp.int32, (vecs, n), 1)

    def stack(lines):
        result = jnp.zeros((vecs, n), F32)
        for i, l in enumerate(lines):
            result = jnp.where(row_id == i, l, result)
        return jnp.sum(result, axis=1, keepdims=True)

    gram = jnp.zeros((vecs, n), F32)
    for j in range(hist):
        column = stack([line[(min(i, j), max(i, j))] for i in range(hist)])
        gram = jnp.where(col_id == j, column, gram)

    def trial_row(a, carry):
        for m in range(hist):
            hin[m, a] = hin[m, a] + beta_mix * hres[m, a]
        return carry

    lax.fori_loop(0, rows, trial_row, 0)

    def freq2(positions):
        f = jnp.where(positions < n // 2, positions, positions - n)
        return f * f

    first = freq2(lax.broadcasted_iota(jnp.int32, (n, n), 0))
    lane = lax.broadcasted_iota(jnp.int32, (n, n), 1)
    cell = n * spacing
    for h, q in [(h, q) for h in range(chunks) for q in range(qper)]:
        middle = freq2((lane // width) * width + me * qper + q)
        last = freq2((mg * chunks + h) * width + lane % width)
        squared = first + middle + last
        value = (cell * cell / np.pi) / jnp.maximum(squared, 1).astype(F32)
        kern[h, q] = jnp.where(squared > 0, value, 0.0) * (1.0 / (n * n * n))

    for c in far_copies[2 if square else 0:]:
        c.wait_recv()

    def late_row(a, accs):
        accs = list(accs)
        total = own[chips - 1, a]
        for t in range(far_in.shape[0]):
            total = total + far_in[t, a]
        inp = rin[a]
        res = total - inp
        resn[a] = inp + beta_mix * res
        for s in range(tiles):
            r = res[8 * s:8 * s + 8, :]
            for i in range(hist):
                accs[i] = accs[i] + hres[i, a, 8 * s:8 * s + 8, :] * r
            accs[hist] = accs[hist] + r * r
        return tuple(accs)

    accs = lax.fori_loop(0, rows, late_row, tuple(zero for _ in range(vecs)))
    column = stack([jnp.sum(x, axis=0, keepdims=True) for x in accs])
    as_row = jnp.sum(jnp.where(row_id == col_id, column, 0.0), axis=0, keepdims=True)
    gram = jnp.where(col_id == hist, column, gram)
    gram = jnp.where(row_id == hist, as_row, gram)

    def sum_over(value, source, landing, send, recv, count, index, device_of):
        source[...] = value
        copies = []
        for k in range(1, count):
            c = pltpu.make_async_remote_copy(
                src_ref=source, dst_ref=landing.at[k], send_sem=send.at[k], recv_sem=recv.at[k],
                device_id=device_of((index + k) % count), device_id_type=MESH,
            )
            c.start()
            copies.append(c)
        for c in copies:
            c.wait_recv()
        landing[0] = value
        total = jnp.zeros_like(value)
        for k in range(count):
            total = total + landing[(index - k + count) % count]
        return total, copies

    sent = []
    gram, copies = sum_over(gram, gram_me, gram_b, gb_s, gb_r, nb, me, lambda x: (x, mg))
    sent += copies
    gram, copies = sum_over(gram, gram_me2, gram_g, gg_s, gg_r, ng, mg, lambda x: (me, x))
    sent += copies
    gram = gram * (1.0 / (n * n * n))

    system = jnp.where(col_id == vecs, 1.0, gram)
    for k in range(vecs):
        pivot_row = system[k:k + 1, :] / system[k:k + 1, k:k + 1]
        factor = jnp.where(row_id == k, 0.0, jnp.broadcast_to(system[:, k:k + 1], (vecs, n)))
        system = jnp.where(row_id == k, pivot_row, system - factor * pivot_row)
    solved = system[:, vecs:vecs + 1]
    weights = solved / jnp.sum(solved, axis=0, keepdims=True)
    wide = [jnp.broadcast_to(weights[m:m + 1, :], (cols, n)) for m in range(vecs)]

    def mix_row(a, carry):
        total = wide[hist] * resn[a]
        for m in range(hist):
            total = total + wide[m] * hin[m, a]
        rho_ref[a] = total
        return carry

    lax.fori_loop(0, rows, mix_row, 0)

    cas = cas_ref[...]

    def exchange(source, landing, send, recv, count, index, device_of):
        copies = []
        for k in range(1, count):
            to = (index + k) % count
            c = pltpu.make_async_remote_copy(
                src_ref=source.at[to], dst_ref=landing.at[index], send_sem=send.at[k],
                recv_sem=recv.at[k], device_id=device_of(to), device_id_type=MESH,
            )
            c.start()
            copies.append(c)
        landing[index] = source[index]
        return copies

    def arrive(copies):
        for c in copies:
            c.wait_recv()
        sent.extend(copies)

    on_band = lambda x: (x, mg)
    on_grid = lambda x: (me, x)
    span = range(chunks)

    spec = dot(rho_ref[...].reshape(rows * cols, n), cas)
    chunk = quad * cols
    parts = swap_lane_groups([spec[i * chunk:(i + 1) * chunk] for i in range(groups)], width)
    flights = []
    for h in span:
        for x in range(ng):
            zsend[h, x] = parts[x * chunks + h]
        flights.append(exchange(zsend.at[h], zrecv.at[h], f1_s.at[h], f1_r.at[h], ng, mg, on_grid))

    nexts = []
    for h in span:
        arrive(flights[h])
        for u in range(quad):
            block = jnp.concatenate([zrecv[h, x, u * cols:(u + 1) * cols, :] for x in range(ng)], axis=0)
            spec = dot(cas, block)
            parts = swap_lane_groups([spec[j * width:(j + 1) * width] for j in range(groups)], width)
            for i in range(groups):
                vsend[h, :, :, i * quad + u, :] = parts[i].reshape(nb, qper, n)
        nexts.append(exchange(vsend.at[h], wrecv.at[h], f2_s.at[h], f2_r.at[h], nb, me, on_band))

    flights = []
    for h in span:
        arrive(nexts[h])
        for q in range(qper):
            spec = dot(cas, wrecv[h, :, q].reshape(n, n)) * kern[h, q]
            wsend[h, :, q] = dot(cas, spec).reshape(nb, rows, n)
        flights.append(exchange(wsend.at[h], vrecv.at[h], b2_s.at[h], b2_r.at[h], nb, me, on_band))

    nexts = []
    for h in span:
        arrive(flights[h])
        for u in range(quad):
            parts = swap_lane_groups(
                [vrecv[h, :, :, i * quad + u, :].reshape(width, n) for i in range(groups)], width
            )
            back = dot(cas, jnp.concatenate(parts, axis=0))
            for x in range(ng):
                z2send[h, x, u * cols:(u + 1) * cols, :] = back[x * cols:(x + 1) * cols]
        nexts.append(exchange(z2send.at[h], y2recv.at[h], b1_s.at[h], b1_r.at[h], ng, mg, on_grid))

    for h in span:
        arrive(nexts[h])
    parts = swap_lane_groups([y2recv[j % chunks, j // chunks] for j in range(groups)], width)
    for i in range(groups):
        pot_ref[i * quad:(i + 1) * quad] = dot(parts[i], cas).reshape(quad, cols, n)

    for c in pair_copies + far_copies + sent:
        c.wait_send()


def cuts(nb, ng, rows, n):
    chunks = 2 if rows % (2 * ng) == 0 and n % (2 * ng * nb) == 0 else 1
    return chunks, n // (ng * chunks)


def local(nb, ng, orbitals, occupations, rho_in, hist_in, hist_res):
    bands = orbitals.shape[0]
    rows, cols, n = rho_in.shape
    hist = hist_in.shape[0]
    vecs = hist + 1
    chips = nb // 2
    chunks, width = cuts(nb, ng, rows, n)
    qper = width // nb
    quad = rows // (ng * chunks)
    fars = 2 if chips == 4 else chips - 1
    dma = pltpu.SemaphoreType.DMA
    vmem = lambda *shape: pltpu.VMEM(shape, F32)
    anywhere = pl.BlockSpec(memory_space=pl.ANY)
    block = jax.ShapeDtypeStruct((rows, cols, n), F32)
    return pl.pallas_call(
        functools.partial(body, nb, ng),
        out_shape=(block, block),
        in_specs=[pl.BlockSpec(memory_space=pltpu.SMEM)] + [anywhere] * 5,
        out_specs=(pl.BlockSpec(memory_space=pltpu.VMEM),) * 2,
        scratch_shapes=[
            pltpu.VMEM((nb, bands, rows, cols, n), orbitals.dtype),
            vmem(rows, cols, n),
            vmem(n, n),
            vmem(hist, rows, cols, n),
            vmem(hist, rows, cols, n),
            vmem(chips, rows, cols, n),
            vmem(chips, rows, cols, n),
            vmem(chips, rows, cols, n),
            vmem(fars, rows, cols, n),
            vmem(2, rows // 2, cols, n),
            vmem(rows, cols, n),
            vmem(vecs, n),
            vmem(nb, vecs, n),
            vmem(vecs, n),
            vmem(ng, vecs, n),
            vmem(chunks, qper, n, n),
            vmem(chunks, ng, quad * cols, n),
            vmem(chunks, ng, quad * cols, n),
            vmem(chunks, nb, qper, rows, n),
            vmem(chunks, nb, qper, rows, n),
            vmem(chunks, nb, qper, rows, n),
            vmem(chunks, nb, qper, rows, n),
            vmem(chunks, ng, quad * cols, n),
            vmem(chunks, ng, quad * cols, n),
            dma((4,)), dma((nb,)),
            dma((chips,)), dma((chips,)), dma((max(chips, 6),)), dma((max(chips, 6),)),
            dma((nb,)), dma((nb,)), dma((ng,)), dma((ng,)),
            dma((chunks, ng)), dma((chunks, ng)), dma((chunks, nb)), dma((chunks, nb)),
            dma((chunks, nb)), dma((chunks, nb)), dma((chunks, ng)), dma((chunks, ng)),
        ],
        compiler_params=pltpu.CompilerParams(collective_id=0, has_side_effects=True, vmem_limit_bytes=67043328),
        name="density_mix_hartree",
    )(occupations, orbitals, rho_in, hist_in, hist_res, jnp.asarray(cas_table(n)))


def solution(mesh):
    return jax.shard_map(
        functools.partial(local, mesh.shape["band"], mesh.shape["grid"]),
        mesh=mesh,
        in_specs=(
            P("band", None, "grid", None),
            P("band"),
            P("band", "grid", None),
            P(None, "band", "grid", None),
            P(None, "band", "grid", None),
        ),
        out_specs=(P("band", "grid", None), P("band", "grid", None)),
        check_vma=False,
    )
```

```python
import functools

import jax
import jax.numpy as jnp
import numpy as np
from jax import lax
from jax.experimental import pallas as pl
from jax.experimental.pallas import tpu as pltpu
from jax.sharding import PartitionSpec as P

beta_mix = 0.5
spacing = 0.2
MESH = pl.DeviceIdType.MESH
F32 = jnp.float32


def cas_table(length):
    phases = np.outer(np.arange(length), np.arange(length)) % length
    angles = phases.astype(np.float64) * (2.0 * np.pi / length)
    return (np.cos(angles) + np.sin(angles)).astype(np.float32)


def dot(left, right):
    half = jnp.bfloat16
    left_top, right_top = left.astype(half), right.astype(half)
    left_rest = (left - left_top.astype(F32)).astype(half)
    right_rest = (right - right_top.astype(F32)).astype(half)
    times = lambda a, b: jnp.dot(a, b, preferred_element_type=F32)
    return times(left_top, right_top) + (times(left_top, right_rest) + times(left_rest, right_top))


def swap_lane_groups(parts, width):
    count = len(parts)
    total = count * width
    group = lax.broadcasted_iota(jnp.int32, parts[0].shape, 1) // width
    step = 1
    while step < count:
        odd = (group // step) % 2 == 1
        mixed = []
        for i in range(count):
            if (i // step) % 2 == 0:
                mixed.append(jnp.where(odd, pltpu.roll(parts[i + step], step * width, 1), parts[i]))
            else:
                mixed.append(jnp.where(odd, parts[i], pltpu.roll(parts[i - step], total - step * width, 1)))
        parts = mixed
        step *= 2
    return parts


def body(
    nb, ng,
    occ, orb_hbm, rho_hbm, hin_hbm, hres_hbm, cas_hbm,
    rho_ref, pot_ref,
    orb, rin, cas_ref, hin, hres, other, own, pair_in, far_in, relay_in, resn,
    gram_me, gram_b, gram_me2, gram_g, kern,
    zsend, zrecv, vsend, wrecv, wsend, vrecv, z2send, y2recv,
    load_sem, orb_sem,
    pair_s, pair_r, far_s, far_r, gb_s, gb_r, gg_s, gg_r,
    f1_s, f1_r, f2_s, f2_r, b2_s, b2_r, b1_s, b1_r,
):
    me = lax.axis_index("band")
    mg = lax.axis_index("grid")
    bands, rows, cols, n = orb.shape[1], orb.shape[2], orb.shape[3], orb.shape[4]
    hist = hin.shape[0]
    vecs = hist + 1
    chips = nb // 2
    chip, core = me // 2, me % 2
    partner = chip * 2 + (1 - core)
    chunks, width = cuts(nb, ng, rows, n)
    groups = ng * chunks
    quad = rows // groups
    qper = width // nb
    square = chips == 4
    order = [d for d in range(chips // 2, 0, -1)] + [d for d in range(chips // 2 + 1, chips)] + [0]

    barrier = pltpu.get_barrier_semaphore()
    for k in range(1, nb):
        pl.semaphore_signal(barrier, inc=1, device_id=((me + k) % nb, mg), device_id_type=MESH)
    for k in range(1, ng):
        pl.semaphore_signal(barrier, inc=1, device_id=(me, (mg + k) % ng), device_id_type=MESH)

    chip_y, chip_x = chip // 2, chip % 2
    x_chip, y_chip = chip_y * 2 + 1 - chip_x, (1 - chip_y) * 2 + chip_x
    opposite = (1 - chip_y) * 2 + 1 - chip_x

    def target_of(t):
        return (opposite, x_chip, y_chip, chip)[t] if square else (chip + order[t]) % chips

    def slab_of(t, mine):
        target = target_of(t)
        return target * 2 + (core if mine else 1 - core)

    orb_loads = []
    for t in range(chips):
        for mine in (False, True):
            s = slab_of(t, mine)
            c = pltpu.make_async_copy(
                orb_hbm.at[:, pl.ds(s * rows, rows)], orb.at[2 * t + mine], orb_sem.at[2 * t + mine]
            )
            c.start()
            orb_loads.append(c)
    loads = [
        pltpu.make_async_copy(hres_hbm, hres, load_sem.at[0]),
        pltpu.make_async_copy(hin_hbm, hin, load_sem.at[1]),
        pltpu.make_async_copy(rho_hbm, rin, load_sem.at[2]),
        pltpu.make_async_copy(cas_hbm, cas_ref, load_sem.at[3]),
    ]
    for c in loads:
        c.start()

    def density(index, out):
        def row(a, carry):
            total = None
            for k in range(bands):
                o = orb[index, k, a].astype(F32)
                term = occ[k] * (o * o)
                total = term if total is None else total + term
            out[a] = total
            return carry

        lax.fori_loop(0, rows, row, 0)

    pair_copies, far_copies = [], []

    def finish(t):
        pair_copies[t].wait_recv()

        def row(a, carry):
            own[t, a] = own[t, a] + pair_in[t, a]
            return carry

        lax.fori_loop(0, rows, row, 0)
        if square:
            if t == 0:
                far(own.at[0, :half], relay_in.at[0], 0, x_chip)
                far(own.at[0, half:], relay_in.at[1], 1, y_chip)
            if t == 1:
                far(own.at[1, :half], far_in.at[0, :half], 2, x_chip)
            if t == 2:
                far(own.at[2, half:], far_in.at[1, half:], 3, y_chip)
        elif order[t]:
            far(own.at[t], far_in.at[t], t, target_of(t))

    half = rows // 2

    def far(source, landing, slot, target):
        c = pltpu.make_async_remote_copy(
            src_ref=source, dst_ref=landing, send_sem=far_s.at[slot], recv_sem=far_r.at[slot],
            device_id=(target * 2 + core, mg), device_id_type=MESH,
        )
        c.start()
        far_copies.append(c)

    def relay():
        def add(side, slab, base):
            def row(a, carry):
                own[slab, base + a] = own[slab, base + a] + relay_in[side, a]
                return carry

            lax.fori_loop(0, half, row, 0)

        far_copies[1].wait_recv()
        add(1, 1, half)
        far(own.at[1, half:], far_in.at[0, half:], 4, x_chip)
        far_copies[0].wait_recv()
        add(0, 2, 0)
        far(own.at[2, :half], far_in.at[1, :half], 5, y_chip)

    for t in range(chips):
        orb_loads[2 * t].wait()
        density(2 * t, other.at[t])
        if t == 0:
            pl.semaphore_wait(barrier, nb - 1 + ng - 1)
        c = pltpu.make_async_remote_copy(
            src_ref=other.at[t], dst_ref=pair_in.at[t], send_sem=pair_s.at[t], recv_sem=pair_r.at[t],
            device_id=(partner, mg), device_id_type=MESH,
        )
        c.start()
        pair_copies.append(c)
        orb_loads[2 * t + 1].wait()
        density(2 * t + 1, own.at[t])
        if t:
            finish(t - 1)
    finish(chips - 1)
    if square:
        relay()

    for c in loads:
        c.wait()
    tiles = cols // 8
    pairs = [(i, j) for i in range(hist) for j in range(i, hist)]

    def gram_row(a, accs):
        accs = list(accs)
        for s in range(tiles):
            vals = [hres[i, a, 8 * s:8 * s + 8, :] for i in range(hist)]
            for x, (i, j) in enumerate(pairs):
                accs[x] = accs[x] + vals[i] * vals[j]
        return tuple(accs)

    zero = jnp.zeros((8, n), F32)
    accs = lax.fori_loop(0, rows, gram_row, tuple(zero for _ in pairs))
    line = {p: jnp.sum(accs[x], axis=0, keepdims=True) for x, p in enumerate(pairs)}
    row_id = lax.broadcasted_iota(jnp.int32, (vecs, n), 0)
    col_id = lax.broadcasted_iota(jnp.int32, (vecs, n), 1)

    def stack(lines):
        result = jnp.zeros((vecs, n), F32)
        for i, l in enumerate(lines):
            result = jnp.where(row_id == i, l, result)
        return jnp.sum(result, axis=1, keepdims=True)

    gram = jnp.zeros((vecs, n), F32)
    for j in range(hist):
        column = stack([line[(min(i, j), max(i, j))] for i in range(hist)])
        gram = jnp.where(col_id == j, column, gram)

    def trial_row(a, carry):
        for m in range(hist):
            hin[m, a] = hin[m, a] + beta_mix * hres[m, a]
        return carry

    lax.fori_loop(0, rows, trial_row, 0)

    def freq2(positions):
        f = jnp.where(positions < n // 2, positions, positions - n)
        return f * f

    first = freq2(lax.broadcasted_iota(jnp.int32, (n, n), 0))
    lane = lax.broadcasted_iota(jnp.int32, (n, n), 1)
    cell = n * spacing
    for h, q in [(h, q) for h in range(chunks) for q in range(qper)]:
        middle = freq2((lane // width) * width + me * qper + q)
        last = freq2((mg * chunks + h) * width + lane % width)
        squared = first + middle + last
        value = (cell * cell / np.pi) / jnp.maximum(squared, 1).astype(F32)
        kern[h, q] = jnp.where(squared > 0, value, 0.0) * (1.0 / (n * n * n))

    for c in far_copies[2 if square else 0:]:
        c.wait_recv()

    def late_row(a, accs):
        accs = list(accs)
        total = own[chips - 1, a]
        for t in range(far_in.shape[0]):
            total = total + far_in[t, a]
        inp = rin[a]
        res = total - inp
        resn[a] = inp + beta_mix * res
        for s in range(tiles):
            r = res[8 * s:8 * s + 8, :]
            for i in range(hist):
                accs[i] = accs[i] + hres[i, a, 8 * s:8 * s + 8, :] * r
            accs[hist] = accs[hist] + r * r
        return tuple(accs)

    accs = lax.fori_loop(0, rows, late_row, tuple(zero for _ in range(vecs)))
    column = stack([jnp.sum(x, axis=0, keepdims=True) for x in accs])
    as_row = jnp.sum(jnp.where(row_id == col_id, column, 0.0), axis=0, keepdims=True)
    gram = jnp.where(col_id == hist, column, gram)
    gram = jnp.where(row_id == hist, as_row, gram)

    def sum_over(value, source, landing, send, recv, count, index, device_of):
        source[...] = value
        copies = []
        for k in range(1, count):
            c = pltpu.make_async_remote_copy(
                src_ref=source, dst_ref=landing.at[k], send_sem=send.at[k], recv_sem=recv.at[k],
                device_id=device_of((index + k) % count), device_id_type=MESH,
            )
            c.start()
            copies.append(c)
        for c in copies:
            c.wait_recv()
        landing[0] = value
        total = jnp.zeros_like(value)
        for k in range(count):
            total = total + landing[(index - k + count) % count]
        return total, copies

    sent = []
    gram, copies = sum_over(gram, gram_me, gram_b, gb_s, gb_r, nb, me, lambda x: (x, mg))
    sent += copies
    gram, copies = sum_over(gram, gram_me2, gram_g, gg_s, gg_r, ng, mg, lambda x: (me, x))
    sent += copies
    gram = gram * (1.0 / (n * n * n))

    system = jnp.where(col_id == vecs, 1.0, gram)
    for k in range(vecs):
        pivot_row = system[k:k + 1, :] / system[k:k + 1, k:k + 1]
        factor = jnp.where(row_id == k, 0.0, jnp.broadcast_to(system[:, k:k + 1], (vecs, n)))
        system = jnp.where(row_id == k, pivot_row, system - factor * pivot_row)
    solved = system[:, vecs:vecs + 1]
    weights = solved / jnp.sum(solved, axis=0, keepdims=True)
    wide = [jnp.broadcast_to(weights[m:m + 1, :], (cols, n)) for m in range(vecs)]

    def mix_row(a, carry):
        total = wide[hist] * resn[a]
        for m in range(hist):
            total = total + wide[m] * hin[m, a]
        rho_ref[a] = total
        return carry

    lax.fori_loop(0, rows, mix_row, 0)

    cas = cas_ref[...]

    def exchange(source, landing, send, recv, count, index, device_of):
        copies = []
        for k in range(1, count):
            to = (index + k) % count
            c = pltpu.make_async_remote_copy(
                src_ref=source.at[to], dst_ref=landing.at[index], send_sem=send.at[k],
                recv_sem=recv.at[k], device_id=device_of(to), device_id_type=MESH,
            )
            c.start()
            copies.append(c)
        landing[index] = source[index]
        return copies

    def arrive(copies):
        for c in copies:
            c.wait_recv()
        sent.extend(copies)

    on_band = lambda x: (x, mg)
    on_grid = lambda x: (me, x)
    span = range(chunks)

    spec = dot(rho_ref[...].reshape(rows * cols, n), cas)
    chunk = quad * cols
    parts = swap_lane_groups([spec[i * chunk:(i + 1) * chunk] for i in range(groups)], width)
    flights = []
    for h in span:
        for x in range(ng):
            zsend[h, x] = parts[x * chunks + h]
        flights.append(exchange(zsend.at[h], zrecv.at[h], f1_s.at[h], f1_r.at[h], ng, mg, on_grid))

    nexts = []
    for h in span:
        arrive(flights[h])
        for u in range(quad):
            block = jnp.concatenate([zrecv[h, x, u * cols:(u + 1) * cols, :] for x in range(ng)], axis=0)
            spec = dot(cas, block)
            parts = swap_lane_groups([spec[j * width:(j + 1) * width] for j in range(groups)], width)
            for i in range(groups):
                vsend[h, :, :, i * quad + u, :] = parts[i].reshape(nb, qper, n)
        nexts.append(exchange(vsend.at[h], wrecv.at[h], f2_s.at[h], f2_r.at[h], nb, me, on_band))

    flights = []
    for h in span:
        arrive(nexts[h])
        for q in range(qper):
            spec = dot(cas, wrecv[h, :, q].reshape(n, n)) * kern[h, q]
            wsend[h, :, q] = dot(cas, spec).reshape(nb, rows, n)
        flights.append(exchange(wsend.at[h], vrecv.at[h], b2_s.at[h], b2_r.at[h], nb, me, on_band))

    nexts = []
    for h in span:
        arrive(flights[h])
        for u in range(quad):
            parts = swap_lane_groups(
                [vrecv[h, :, :, i * quad + u, :].reshape(width, n) for i in range(groups)], width
            )
            back = dot(cas, jnp.concatenate(parts, axis=0))
            for x in range(ng):
                z2send[h, x, u * cols:(u + 1) * cols, :] = back[x * cols:(x + 1) * cols]
        nexts.append(exchange(z2send.at[h], y2recv.at[h], b1_s.at[h], b1_r.at[h], ng, mg, on_grid))

    for h in span:
        arrive(nexts[h])
    parts = swap_lane_groups([y2recv[j % chunks, j // chunks] for j in range(groups)], width)
    for i in range(groups):
        pot_ref[i * quad:(i + 1) * quad] = dot(parts[i], cas).reshape(quad, cols, n)

    for c in pair_copies + far_copies + sent:
        c.wait_send()


def cuts(nb, ng, rows, n):
    chunks = 2 if rows % (2 * ng) == 0 and n % (2 * ng * nb) == 0 else 1
    return chunks, n // (ng * chunks)


def local(nb, ng, orbitals, occupations, rho_in, hist_in, hist_res):
    bands = orbitals.shape[0]
    rows, cols, n = rho_in.shape
    hist = hist_in.shape[0]
    vecs = hist + 1
    chips = nb // 2
    chunks, width = cuts(nb, ng, rows, n)
    qper = width // nb
    quad = rows // (ng * chunks)
    fars = 2 if chips == 4 else chips - 1
    dma = pltpu.SemaphoreType.DMA
    vmem = lambda *shape: pltpu.VMEM(shape, F32)
    anywhere = pl.BlockSpec(memory_space=pl.ANY)
    block = jax.ShapeDtypeStruct((rows, cols, n), F32)
    results = pl.pallas_call(
        functools.partial(body, nb, ng),
        out_shape=(block, block),
        in_specs=[pl.BlockSpec(memory_space=pltpu.SMEM)] + [anywhere] * 5,
        out_specs=(pl.BlockSpec(memory_space=pltpu.VMEM),) * 2,
        scratch_shapes=[
            pltpu.VMEM((nb, bands, rows, cols, n), orbitals.dtype),
            vmem(rows, cols, n),
            vmem(n, n),
            vmem(hist, rows, cols, n),
            vmem(hist, rows, cols, n),
            vmem(chips, rows, cols, n),
            vmem(chips, rows, cols, n),
            vmem(chips, rows, cols, n),
            vmem(fars, rows, cols, n),
            vmem(2, rows // 2, cols, n),
            vmem(rows, cols, n),
            vmem(vecs, n),
            vmem(nb, vecs, n),
            vmem(vecs, n),
            vmem(ng, vecs, n),
            vmem(chunks, qper, n, n),
            vmem(chunks, ng, quad * cols, n),
            vmem(chunks, ng, quad * cols, n),
            vmem(chunks, nb, qper, rows, n),
            vmem(chunks, nb, qper, rows, n),
            vmem(chunks, nb, qper, rows, n),
            vmem(chunks, nb, qper, rows, n),
            vmem(chunks, ng, quad * cols, n),
            vmem(chunks, ng, quad * cols, n),
            dma((4,)), dma((nb,)),
            dma((chips,)), dma((chips,)), dma((max(chips, 6),)), dma((max(chips, 6),)),
            dma((nb,)), dma((nb,)), dma((ng,)), dma((ng,)),
            dma((chunks, ng)), dma((chunks, ng)), dma((chunks, nb)), dma((chunks, nb)),
            dma((chunks, nb)), dma((chunks, nb)), dma((chunks, ng)), dma((chunks, ng)),
        ],
        compiler_params=pltpu.CompilerParams(collective_id=0, has_side_effects=True, vmem_limit_bytes=67043328),
        name="density_mix_hartree",
    )(occupations, orbitals, rho_in, hist_in, hist_res, jnp.asarray(cas_table(n)))

    def hand_out(rho_from, pot_from, rho_to, pot_to, held, sem):
        pairs = ((rho_from, rho_to), (pot_from, pot_to))
        fetch = [pltpu.make_async_copy(a, held.at[x], sem.at[x]) for x, (a, b) in enumerate(pairs)]
        put = [pltpu.make_async_copy(held.at[x], b, sem.at[2 + x]) for x, (a, b) in enumerate(pairs)]
        for c in fetch:
            c.start()
        for x in range(2):
            fetch[x].wait()
            put[x].start()
        for c in put:
            c.wait()

    return pl.pallas_call(
        hand_out,
        out_shape=(block, block),
        in_specs=[anywhere] * 2,
        out_specs=(anywhere,) * 2,
        scratch_shapes=[vmem(2, rows, cols, n), dma((4,))],
        compiler_params=pltpu.CompilerParams(vmem_limit_bytes=67043328),
        name="hand_out",
    )(*results)


def solution(mesh):
    return jax.shard_map(
        functools.partial(local, mesh.shape["band"], mesh.shape["grid"]),
        mesh=mesh,
        in_specs=(
            P("band", None, "grid", None),
            P("band"),
            P("band", "grid", None),
            P(None, "band", "grid", None),
            P(None, "band", "grid", None),
        ),
        out_specs=(P("band", "grid", None), P("band", "grid", None)),
        check_vma=False,
    )
```
